32 devices in a mesh: chan: 8 (over z, core), band: 4 (over y, x).
Axes of the slice: x: 2, y: 2, z: 4, core: 2. Of those that a mesh axis runs over, the one named last changes fastest.
Arguments:
- residual: float32 [64, 96, 16384], P('chan', 'band'), may hold values from -60 to 60
- weight_index: int32 [64], P('chan'), may hold values from 0 to 15
- weight_table: float32 [16], replicated, may hold values from 0.2 to 5
- gridded: float32 [2, 8, 128, 16384], P(None, 'chan', 'band'), may hold values from -6 to 6
Outputs:
- components: float32 [3, 96, 16384], P(None, 'band', 'chan')
- spectrum: float32 [2, 8, 16384, 128], P(None, 'chan', 'band')
The draws below stay inside these ranges and needn't reach their ends.
All inputs are finite; a program needn't handle non-finite values.
Results may differ from the reference program's by a relative error of at most 0.0002.
Values sent between devices are 32-bit elements; how exact they have to be, the bound alone decides.
A program may use at most 128 MiB of HBM per device.

```python
import math
import jax
import jax.numpy as jnp
from jax import lax

IMG = 16384
GRID = 16384
NW = 16
CHANNELS = 64
IMG_ROWS = 96
ROWS = 128
GROUPS = 8


def draw_residual(key, part):
    key_sky, key_noise = jax.random.split(jax.random.fold_in(key, 11), 2)
    position = jnp.arange(CHANNELS, dtype=jnp.float32)
    offset = (2.0 * position + 1.0) / CHANNELS - 1.0
    amplitude = jnp.array([1.0, 0.7, 0.5], dtype=jnp.float32)
    sky = jax.random.normal(key_sky, (3, IMG_ROWS, IMG), jnp.float32) * amplitude[:, None, None]
    noise = 3.0 * jax.random.normal(key_noise, (CHANNELS, IMG_ROWS, IMG), jnp.float32)
    values = sky[0][None] + offset[:, None, None] * sky[1][None] + (offset * offset)[:, None, None] * sky[2][None] + noise
    return jnp.clip(values, -60.0, 60.0)


def touch_ends(entries, rng, smallest, high):
    longest = entries.shape.index(max(entries.shape))
    spots = []
    for shift in (0, 1):
        where = [jax.random.randint(jax.random.fold_in(rng, axis), (), 0, length) for axis, length in enumerate(entries.shape)]
        where[longest] = (where[longest] + shift) % entries.shape[longest]
        spots.append(tuple(where))
    return entries.at[spots[0]].set(smallest).at[spots[1]].set(high)


def levels(stream_key, shape, cuts, low, top_value):
    def one(dim, blocks):
        heights = jax.random.uniform(jax.random.fold_in(jax.random.fold_in(stream_key, 6), dim), (blocks,), jnp.float32, low / len(cuts), top_value / len(cuts))
        return jnp.repeat(jnp.exp(heights), shape[dim] // blocks).reshape((-1,) + (1,) * (len(shape) - dim - 1))

    gain = one(*cuts[0])
    for cut in cuts[1:]:
        gain = gain * one(*cut)
    return gain


def normal_values(stream_key, shape, width, most, cuts=(), kind=jnp.bfloat16):
    values = width * jax.random.normal(stream_key, shape, jnp.float32)
    if cuts:
        values = values * levels(stream_key, shape, cuts, -0.22, 0.18)
    return jnp.clip(values, -most, most).astype(kind)


def setup_inputs(seed: int = 0) -> dict:
    key_of = jax.random.split(jax.random.key(seed), 5)
    return {
        "residual": draw_residual(jax.random.fold_in(key_of[4], 71), 0),
        "weight_index": touch_ends(jax.random.randint(key_of[1], (CHANNELS,), 0, NW), jax.random.fold_in(key_of[1], 1), 0, NW - 1).astype(jnp.int32),
        "weight_table": jnp.clip(jnp.exp(jax.random.uniform(key_of[2], (NW,), jnp.float32, math.log(0.2), math.log(5.0))), 0.2, 5.0),
        "gridded": normal_values(key_of[3], (2, GROUPS, ROWS, GRID), 1.0, 6.0, ((1, 8), (2, 4)), jnp.float32),
    }


def channel_terms(weight_index, weight_table, first, total):
    count = weight_index.shape[0]
    position = (first + jnp.arange(count, dtype=jnp.int32)).astype(jnp.float32)
    offset = (2.0 * position + 1.0) / total - 1.0
    slots = jnp.arange(weight_table.shape[0], dtype=jnp.int32)
    onehot = (weight_index[:, None] == slots[None, :]).astype(jnp.float32)
    weights = jnp.dot(onehot, weight_table, precision=lax.Precision.HIGHEST)
    return (weights, offset)

def solve_terms(moment, taylor):
    sum_zero, sum_one, sum_two, sum_three, sum_four = (moment[0], moment[1], moment[2], moment[3], moment[4])
    entry_aa = sum_two * sum_four - sum_three * sum_three
    entry_ab = sum_two * sum_three - sum_one * sum_four
    entry_ac = sum_one * sum_three - sum_two * sum_two
    entry_bb = sum_zero * sum_four - sum_two * sum_two
    entry_bc = sum_one * sum_two - sum_zero * sum_three
    entry_cc = sum_zero * sum_two - sum_one * sum_one
    determ = sum_zero * entry_aa + sum_one * entry_ab + sum_two * entry_ac
    inverse = jnp.stack([jnp.stack([entry_aa, entry_ab, entry_ac]), jnp.stack([entry_ab, entry_bb, entry_bc]), jnp.stack([entry_ac, entry_bc, entry_cc])]) / determ
    return jnp.einsum('ts,sij->tij', inverse, taylor, precision=lax.Precision.HIGHEST)

def reference(residual, weight_index, weight_table, gridded):
    weights, offset = channel_terms(weight_index, weight_table, 0, CHANNELS)
    coeffs = jnp.stack([weights, weights * offset, weights * offset * offset])
    flat = residual.reshape(residual.shape[0], -1)
    taylor = jnp.dot(coeffs, flat, precision=lax.Precision.HIGHEST).reshape(3, residual.shape[1], residual.shape[2])
    moment = jnp.stack([jnp.sum(weights * offset ** power) for power in range(5)])
    components = solve_terms(moment, taylor)
    field = gridded[0] + 1j * gridded[1]
    transformed = jnp.fft.fft(field, axis=-1) / jnp.sqrt(jnp.float32(GRID))
    stacked = jnp.stack([jnp.real(transformed), jnp.imag(transformed)]).astype(jnp.float32)
    spectrum = jnp.swapaxes(stacked, 2, 3)
    return (components, spectrum)
```

```python
import functools
import math

import jax
import jax.numpy as jnp
import numpy as np
from jax import lax
from jax.experimental import pallas as pl
from jax.experimental.pallas import tpu as pltpu
from jax.sharding import PartitionSpec as P

MESH = pl.DeviceIdType.MESH
LANES = 128
SUB = 8


def block_form(table):
    real = np.block([[table.real, -table.imag], [table.imag, table.real]]).astype(np.float32)
    high = real.astype(jnp.bfloat16)
    low = (real - high.astype(np.float32)).astype(jnp.bfloat16)
    return np.concatenate([high, low, high], axis=1)


def dft(size):
    grid = np.outer(np.arange(size), np.arange(size)) % size
    return np.exp(-2j * np.pi * grid / size)


def tables(length):
    outer = length // LANES
    turn = np.exp(-2j * np.pi * np.outer(np.arange(outer), np.arange(LANES)) / length)
    turn = turn / math.sqrt(length)
    return (
        block_form(dft(outer)),
        block_form(dft(LANES)),
        turn.real.astype(np.float32),
        turn.imag.astype(np.float32),
    )


def solve_terms(moment, taylor):
    s0, s1, s2, s3, s4 = (moment[j, 0] for j in range(5))
    aa = s2 * s4 - s3 * s3
    ab = s2 * s3 - s1 * s4
    ac = s1 * s3 - s2 * s2
    bb = s0 * s4 - s2 * s2
    bc = s1 * s2 - s0 * s3
    cc = s0 * s2 - s1 * s1
    determ = s0 * aa + s1 * ab + s2 * ac
    rows = ((aa, ab, ac), (ab, bb, bc), (ac, bc, cc))
    return jnp.stack(
        [sum((entry / determ) * taylor[s] for s, entry in enumerate(row)) for row in rows]
    )


def exchange_kernel(
    nc,
    nb,
    idx_ref,
    tab_ref,
    first_ref,
    second_ref,
    turn_re_ref,
    turn_im_ref,
    res_hbm,
    grid_hbm,
    spec_hbm,
    tay_ref,
    mom_ref,
    grid_v,
    out_v,
    res_v,
    part_v,
    mom_own,
    mom_all,
    *rest,
):
    steps = int(math.log2(nc))
    lands = rest[:steps]
    (grid_sem, res_sem, own_sem, fs_sem, fr_sem, rs_sem, rr_sem, ms_sem, mr_sem) = rest[steps:]
    chan = lax.axis_index("chan")
    band = lax.axis_index("band")
    tiles, outer8 = grid_v.shape[1], grid_v.shape[2]
    outer = outer8 // SUB
    rows = tiles * SUB
    kept = LANES // nb
    parts = res_v.shape[0]
    count = res_v.shape[1]
    wide = part_v.shape[3]

    def grid_copy(t):
        return pltpu.make_async_copy(grid_hbm.at[:, t], grid_v.at[:, t], grid_sem.at[t])

    def res_copy(c):
        return pltpu.make_async_copy(
            res_hbm.at[:, pl.ds(c * SUB, SUB), :], res_v.at[c], res_sem.at[c]
        )

    order = max(tiles, parts)
    for i in range(order):
        if i < tiles:
            grid_copy(i).start()
        if i < parts:
            res_copy(i).start()

    barrier = pltpu.get_barrier_semaphore()
    for d in range(1, nc):
        peer = lax.rem(chan + d, nc)
        pl.semaphore_signal(barrier, inc=1, device_id=(peer, band), device_id_type=MESH)
    for d in range(1, nb):
        peer = lax.rem(band + d, nb)
        pl.semaphore_signal(barrier, inc=1, device_id=(chan, peer), device_id_type=MESH)

    total = count * nc
    coeffs = []
    moments = [jnp.float32(0.0)] * 5
    for c in range(count):
        weight = tab_ref[idx_ref[c]]
        position = (chan * count + c).astype(jnp.float32)
        offset = (2.0 * position + 1.0) * (1.0 / total) - 1.0
        power = weight
        trio = []
        for j in range(5):
            if j < 3:
                trio.append(power)
            moments[j] = moments[j] + power
            power = power * offset
        coeffs.append(trio)
    line = lax.broadcasted_iota(jnp.int32, (SUB, LANES), 0)
    tile = jnp.zeros((SUB, LANES), jnp.float32)
    for j in range(5):
        tile = jnp.where(line == j, moments[j], tile)
    mom_own[...] = tile

    def transform(t):
        def pair(i, carry):
            cols = []
            for k in range(2):
                r = i * 2 + k
                cols.append(
                    jnp.concatenate(
                        [grid_v[p, t, pl.ds(r, outer, stride=SUB), :] for p in range(2)], axis=0
                    )
                )
            x = jnp.concatenate(cols, axis=1)
            high = x.astype(jnp.bfloat16)
            low = (x - high.astype(jnp.float32)).astype(jnp.bfloat16)
            mid = jnp.dot(
                first_ref[...],
                jnp.concatenate([high, high, low], axis=0),
                preferred_element_type=jnp.float32,
            )
            turn_re, turn_im = turn_re_ref[...], turn_im_ref[...]
            turned = []
            for k in range(2):
                re = mid[:outer, k * LANES : (k + 1) * LANES]
                im = mid[outer:, k * LANES : (k + 1) * LANES]
                turned.append(
                    jnp.concatenate(
                        [re * turn_re - im * turn_im, re * turn_im + im * turn_re], axis=1
                    )
                )
            y = jnp.concatenate(turned, axis=0)
            high = y.astype(jnp.bfloat16)
            low = (y - high.astype(jnp.float32)).astype(jnp.bfloat16)
            out = lax.dot_general(
                second_ref[...],
                jnp.concatenate([high, high, low], axis=1),
                (((1,), (1,)), ((), ())),
                preferred_element_type=jnp.float32,
            )
            for k in range(2):
                for p in range(2):
                    out_v[p, t * SUB + i * 2 + k] = out[
                        p * LANES : (p + 1) * LANES, k * outer : (k + 1) * outer
                    ]
            return carry

        lax.fori_loop(0, SUB // 2, pair, 0)

    def block_send(t, d):
        peer = lax.rem(band + d, nb)
        return pltpu.make_async_remote_copy(
            src_ref=out_v.at[:, pl.ds(t * SUB, SUB), pl.ds(peer * kept, kept), :],
            dst_ref=spec_hbm.at[:, pl.ds(band * rows + t * SUB, SUB), :, :],
            send_sem=fs_sem.at[t, d - 1],
            recv_sem=fr_sem.at[t, d - 1],
            device_id=(chan, peer),
            device_id_type=MESH,
        )

    def block_keep(t):
        return pltpu.make_async_copy(
            out_v.at[:, pl.ds(t * SUB, SUB), pl.ds(band * kept, kept), :],
            spec_hbm.at[:, pl.ds(band * rows + t * SUB, SUB), :, :],
            own_sem.at[t],
        )

    def weigh(c):
        step = 512 if wide % 512 == 0 else LANES

        def one(j, carry):
            spot = 0
            for s in range(steps):
                spot = spot + ((j // (1 << s)) % 2) * (1 << (steps - 1 - s))
            for q in range(wide // step):
                col = pl.multiple_of(j * wide + q * step, LANES)
                sums = [None] * 3
                for ch in range(count):
                    x = res_v[c, ch, :, pl.ds(col, step)]
                    for t in range(3):
                        term = coeffs[ch][t] * x
                        sums[t] = term if ch == 0 else sums[t] + term
                for t in range(3):
                    part_v[c, spot, pl.ds(t * SUB, SUB), pl.ds(q * step, step)] = sums[t]
            return carry

        lax.fori_loop(0, nc, one, 0)

    bits = [(chan // (1 << s)) % 2 for s in range(steps)]
    partners = [chan + (1 - 2 * bits[s]) * (1 << s) for s in range(steps)]
    starts = [0]
    for s in range(steps):
        starts.append(starts[s] + bits[s] * (nc >> (s + 1)))

    def half_send(c, s):
        size = nc >> (s + 1)
        begin = starts[s] + (1 - bits[s]) * size
        return pltpu.make_async_remote_copy(
            src_ref=part_v.at[c, pl.ds(begin, size)],
            dst_ref=lands[s].at[c],
            send_sem=rs_sem.at[c, s],
            recv_sem=rr_sem.at[c, s],
            device_id=(partners[s], band),
            device_id_type=MESH,
        )

    def half_add(c, s):
        half_send(c, s).wait_recv()
        size = nc >> (s + 1)
        if s == steps - 1:
            for t in range(3):
                span = pl.ds(t * SUB, SUB)
                tay_ref[t, c] = part_v[c, starts[s + 1], span, :] + lands[s][c, 0, span, :]
            return
        half = size // 2
        for mine in (1 - bits[s + 1], bits[s + 1]):
            for q in range(half):
                at = mine * half + q
                part_v[c, starts[s + 1] + at] = part_v[c, starts[s + 1] + at] + lands[s][c, at]
            if mine is not bits[s + 1]:
                half_send(c, s + 1).start()

    def mom_send(d):
        peer = lax.rem(chan + d, nc)
        return pltpu.make_async_remote_copy(
            src_ref=mom_own,
            dst_ref=mom_all.at[d - 1],
            send_sem=ms_sem.at[d - 1],
            recv_sem=mr_sem.at[d - 1],
            device_id=(peer, band),
            device_id_type=MESH,
        )

    for i in range(order):
        if i < tiles:
            grid_copy(i).wait()
            transform(i)
            if i == 0:
                pl.semaphore_wait(barrier, nc + nb - 2)
            for d in range(1, nb):
                block_send(i, d).start()
            block_keep(i).start()
        if i < parts:
            res_copy(i).wait()
            weigh(i)
            half_send(i, 0).start()
        if 1 <= i <= parts:
            half_add(i - 1, 0)
    if parts >= order:
        half_add(parts - 1, 0)
    for d in range(1, nc):
        mom_send(d).start()
    for s in range(1, steps):
        for c in range(parts):
            half_add(c, s)
    moment = mom_own[...]
    for d in range(1, nc):
        mom_send(d).wait_recv()
        moment = moment + mom_all[d - 1]
    mom_ref[...] = moment
    for d in range(1, nc):
        mom_send(d).wait_send()
    for c in range(parts):
        for s in range(steps):
            half_send(c, s).wait_send()
    for t in range(tiles):
        block_keep(t).wait()
        for d in range(1, nb):
            block_send(t, d).wait()


def turn_kernel(in_ref, out_ref):
    many, outer = in_ref.shape[2], in_ref.shape[3]
    for k in range(many):
        out_ref[0, 0, pl.ds(k * outer, outer), :] = in_ref[0, :, k, :].T


def local(nc, nb, residual, weight_index, weight_table, gridded):
    count, row_count, columns = residual.shape
    _, groups, rows, length = gridded.shape
    outer = length // LANES
    tiles, parts = rows // SUB, row_count // SUB
    wide = columns // nc
    kept = LANES // nb
    steps = int(math.log2(nc))
    view = gridded.reshape(2, tiles, SUB, outer, LANES)
    view = jnp.transpose(view, (0, 1, 3, 2, 4)).reshape(2, tiles, outer * SUB, LANES)
    vmem = pl.BlockSpec(memory_space=pltpu.VMEM)
    smem = pl.BlockSpec(memory_space=pltpu.SMEM)
    hbm = pl.BlockSpec(memory_space=pl.ANY)
    dma = pltpu.SemaphoreType.DMA
    raw, taylor, moment = pl.pallas_call(
        functools.partial(exchange_kernel, nc, nb),
        out_shape=(
            jax.ShapeDtypeStruct((2, nb * rows, kept, outer), jnp.float32),
            jax.ShapeDtypeStruct((3, parts, SUB, wide), jnp.float32),
            jax.ShapeDtypeStruct((SUB, LANES), jnp.float32),
        ),
        in_specs=[smem, smem, vmem, vmem, vmem, vmem, hbm, hbm],
        out_specs=(hbm, vmem, vmem),
        scratch_shapes=[
            pltpu.VMEM((2, tiles, outer * SUB, LANES), jnp.float32),
            pltpu.VMEM((2, rows, LANES, outer), jnp.float32),
            pltpu.VMEM((parts, count, SUB, columns), jnp.float32),
            pltpu.VMEM((parts, nc, 3 * SUB, wide), jnp.float32),
            pltpu.VMEM((SUB, LANES), jnp.float32),
            pltpu.VMEM((nc - 1, SUB, LANES), jnp.float32),
            *[
                pltpu.VMEM((parts, nc >> (s + 1), 3 * SUB, wide), jnp.float32)
                for s in range(steps)
            ],
            dma((tiles,)),
            dma((parts,)),
            dma((tiles,)),
            dma((tiles, nb - 1)),
            dma((tiles, nb - 1)),
            dma((parts, steps)),
            dma((parts, steps)),
            dma((nc - 1,)),
            dma((nc - 1,)),
        ],
        compiler_params=pltpu.CompilerParams(
            collective_id=0, has_side_effects=True, vmem_limit_bytes=60 * 1024 * 1024
        ),
        name="exchange",
    )(weight_index, weight_table, *map(jnp.asarray, tables(length)), residual, view)
    many = min(SUB, kept)
    spectrum = pl.pallas_call(
        turn_kernel,
        grid=(2, kept // many),
        out_shape=jax.ShapeDtypeStruct((2, 1, kept * outer, nb * rows), jnp.float32),
        in_specs=[pl.BlockSpec((1, nb * rows, many, outer), lambda p, k: (p, 0, k, 0))],
        out_specs=pl.BlockSpec((1, 1, many * outer, nb * rows), lambda p, k: (p, 0, k, 0)),
        name="turn",
    )(raw)
    components = solve_terms(moment, taylor.reshape(3, row_count, wide))
    return (components, spectrum)


def solution(mesh):
    nc, nb = mesh.shape["chan"], mesh.shape["band"]
    in_specs = (P("chan", "band", None), P("chan"), P(), P(None, "chan", "band", None))
    out_specs = (P(None, "band", "chan"), P(None, "chan", "band", None))
    return jax.shard_map(
        functools.partial(local, nc, nb),
        mesh=mesh,
        in_specs=in_specs,
        out_specs=out_specs,
        check_vma=False,
    )
```

```python
import functools
import math

import jax
import jax.numpy as jnp
import numpy as np
from jax import lax
from jax.experimental import pallas as pl
from jax.experimental.pallas import tpu as pltpu
from jax.sharding import PartitionSpec as P

MESH = pl.DeviceIdType.MESH
LANES = 128
SUB = 8


def block_form(table):
    real = np.block([[table.real, -table.imag], [table.imag, table.real]]).astype(np.float32)
    high = real.astype(jnp.bfloat16)
    low = (real - high.astype(np.float32)).astype(jnp.bfloat16)
    return np.concatenate([high, low, high], axis=1)


def dft(size):
    grid = np.outer(np.arange(size), np.arange(size)) % size
    return np.exp(-2j * np.pi * grid / size)


def tables(length):
    outer = length // LANES
    turn = np.exp(-2j * np.pi * np.outer(np.arange(outer), np.arange(LANES)) / length)
    turn = turn / math.sqrt(length)
    return (
        block_form(dft(outer)),
        block_form(dft(LANES)),
        turn.real.astype(np.float32),
        turn.imag.astype(np.float32),
    )


def inverse_rows(moment):
    s0, s1, s2, s3, s4 = (moment[j : j + 1, :] for j in range(5))
    aa = s2 * s4 - s3 * s3
    ab = s2 * s3 - s1 * s4
    ac = s1 * s3 - s2 * s2
    bb = s0 * s4 - s2 * s2
    bc = s1 * s2 - s0 * s3
    cc = s0 * s2 - s1 * s1
    determ = s0 * aa + s1 * ab + s2 * ac
    return [entry / determ for entry in (aa, ab, ac, bb, bc, cc)]


def exchange_kernel(
    nc,
    nb,
    idx_ref,
    tab_ref,
    first_ref,
    second_ref,
    turn_re_ref,
    turn_im_ref,
    res_hbm,
    grid_hbm,
    spec_hbm,
    tay_ref,
    mom_ref,
    grid_v,
    out_v,
    res_v,
    part_v,
    mom_own,
    mom_all,
    *rest,
):
    steps = int(math.log2(nc))
    lands = rest[:steps]
    (grid_sem, res_sem, own_sem, fs_sem, fr_sem, rs_sem, rr_sem, ms_sem, mr_sem) = rest[steps:]
    chan = lax.axis_index("chan")
    band = lax.axis_index("band")
    tiles, outer8 = grid_v.shape[1], grid_v.shape[2]
    outer = outer8 // SUB
    rows = tiles * SUB
    kept = LANES // nb
    parts = res_v.shape[0]
    count = res_v.shape[1]
    wide = part_v.shape[3]

    def grid_copy(t):
        return pltpu.make_async_copy(grid_hbm.at[:, t], grid_v.at[:, t], grid_sem.at[t])

    def res_copy(c):
        return pltpu.make_async_copy(
            res_hbm.at[:, pl.ds(c * SUB, SUB), :], res_v.at[c], res_sem.at[c]
        )

    order = max(tiles, parts)
    for i in range(order):
        if i < tiles:
            grid_copy(i).start()
        if i < parts:
            res_copy(i).start()

    barrier = pltpu.get_barrier_semaphore()
    for d in range(1, nc):
        peer = lax.rem(chan + d, nc)
        pl.semaphore_signal(barrier, inc=1, device_id=(peer, band), device_id_type=MESH)
    for d in range(1, nb):
        peer = lax.rem(band + d, nb)
        pl.semaphore_signal(barrier, inc=1, device_id=(chan, peer), device_id_type=MESH)

    total = count * nc
    coeffs = []
    moments = [jnp.float32(0.0)] * 5
    for c in range(count):
        weight = tab_ref[idx_ref[c]]
        position = (chan * count + c).astype(jnp.float32)
        offset = (2.0 * position + 1.0) * (1.0 / total) - 1.0
        power = weight
        trio = []
        for j in range(5):
            if j < 3:
                trio.append(power)
            moments[j] = moments[j] + power
            power = power * offset
        coeffs.append(trio)
    line = lax.broadcasted_iota(jnp.int32, (SUB, LANES), 0)
    tile = jnp.zeros((SUB, LANES), jnp.float32)
    for j in range(5):
        tile = jnp.where(line == j, moments[j], tile)
    mom_own[...] = tile

    def transform(t):
        def pair(i, carry):
            cols = []
            for k in range(2):
                r = i * 2 + k
                cols.append(
                    jnp.concatenate(
                        [grid_v[p, t, pl.ds(r, outer, stride=SUB), :] for p in range(2)], axis=0
                    )
                )
            x = jnp.concatenate(cols, axis=1)
            high = x.astype(jnp.bfloat16)
            low = (x - high.astype(jnp.float32)).astype(jnp.bfloat16)
            mid = jnp.dot(
                first_ref[...],
                jnp.concatenate([high, high, low], axis=0),
                preferred_element_type=jnp.float32,
            )
            turn_re, turn_im = turn_re_ref[...], turn_im_ref[...]
            turned = []
            for k in range(2):
                re = mid[:outer, k * LANES : (k + 1) * LANES]
                im = mid[outer:, k * LANES : (k + 1) * LANES]
                turned.append(
                    jnp.concatenate(
                        [re * turn_re - im * turn_im, re * turn_im + im * turn_re], axis=1
                    )
                )
            y = jnp.concatenate(turned, axis=0)
            high = y.astype(jnp.bfloat16)
            low = (y - high.astype(jnp.float32)).astype(jnp.bfloat16)
            out = lax.dot_general(
                second_ref[...],
                jnp.concatenate([high, high, low], axis=1),
                (((1,), (1,)), ((), ())),
                preferred_element_type=jnp.float32,
            )
            for k in range(2):
                for p in range(2):
                    out_v[p, t * SUB + i * 2 + k] = out[
                        p * LANES : (p + 1) * LANES, k * outer : (k + 1) * outer
                    ]
            return carry

        lax.fori_loop(0, SUB // 2, pair, 0)

    def block_send(t, d):
        peer = lax.rem(band + d, nb)
        return pltpu.make_async_remote_copy(
            src_ref=out_v.at[:, pl.ds(t * SUB, SUB), pl.ds(peer * kept, kept), :],
            dst_ref=spec_hbm.at[:, pl.ds(band * rows + t * SUB, SUB), :, :],
            send_sem=fs_sem.at[t, d - 1],
            recv_sem=fr_sem.at[t, d - 1],
            device_id=(chan, peer),
            device_id_type=MESH,
        )

    def block_keep(t):
        return pltpu.make_async_copy(
            out_v.at[:, pl.ds(t * SUB, SUB), pl.ds(band * kept, kept), :],
            spec_hbm.at[:, pl.ds(band * rows + t * SUB, SUB), :, :],
            own_sem.at[t],
        )

    def weigh(c):
        step = 512 if wide % 512 == 0 else LANES

        def one(j, carry):
            spot = 0
            for s in range(steps):
                spot = spot + ((j // (1 << s)) % 2) * (1 << (steps - 1 - s))
            for q in range(wide // step):
                col = pl.multiple_of(j * wide + q * step, LANES)
                sums = [None] * 3
                for ch in range(count):
                    x = res_v[c, ch, :, pl.ds(col, step)]
                    for t in range(3):
                        term = coeffs[ch][t] * x
                        sums[t] = term if ch == 0 else sums[t] + term
                for t in range(3):
                    part_v[c, spot, pl.ds(t * SUB, SUB), pl.ds(q * step, step)] = sums[t]
            return carry

        lax.fori_loop(0, nc, one, 0)

    bits = [(chan // (1 << s)) % 2 for s in range(steps)]
    partners = [chan + (1 - 2 * bits[s]) * (1 << s) for s in range(steps)]
    starts = [0]
    for s in range(steps):
        starts.append(starts[s] + bits[s] * (nc >> (s + 1)))

    def half_send(c, s):
        size = nc >> (s + 1)
        begin = starts[s] + (1 - bits[s]) * size
        return pltpu.make_async_remote_copy(
            src_ref=part_v.at[c, pl.ds(begin, size)],
            dst_ref=lands[s].at[c],
            send_sem=rs_sem.at[c, s],
            recv_sem=rr_sem.at[c, s],
            device_id=(partners[s], band),
            device_id_type=MESH,
        )

    def half_add(c, s):
        half_send(c, s).wait_recv()
        size = nc >> (s + 1)
        if s == steps - 1:
            for t in range(3):
                span = pl.ds(t * SUB, SUB)
                tay_ref[t, c] = part_v[c, starts[s + 1], span, :] + lands[s][c, 0, span, :]
            return
        half = size // 2
        for mine in (1 - bits[s + 1], bits[s + 1]):
            for q in range(half):
                at = mine * half + q
                part_v[c, starts[s + 1] + at] = part_v[c, starts[s + 1] + at] + lands[s][c, at]
            if mine is not bits[s + 1]:
                half_send(c, s + 1).start()

    def mom_send(d):
        peer = lax.rem(chan + d, nc)
        return pltpu.make_async_remote_copy(
            src_ref=mom_own,
            dst_ref=mom_all.at[d - 1],
            send_sem=ms_sem.at[d - 1],
            recv_sem=mr_sem.at[d - 1],
            device_id=(peer, band),
            device_id_type=MESH,
        )

    for i in range(order):
        if i < tiles:
            grid_copy(i).wait()
            transform(i)
            if i == 0:
                pl.semaphore_wait(barrier, nc + nb - 2)
            for d in range(1, nb):
                block_send(i, d).start()
            block_keep(i).start()
        if i < parts:
            res_copy(i).wait()
            weigh(i)
            half_send(i, 0).start()
        if 1 <= i <= parts:
            half_add(i - 1, 0)
    if parts >= order:
        half_add(parts - 1, 0)
    for d in range(1, nc):
        mom_send(d).start()
    for s in range(1, steps):
        for c in range(parts):
            half_add(c, s)
    moment = mom_own[...]
    for d in range(1, nc):
        mom_send(d).wait_recv()
        moment = moment + mom_all[d - 1]
    entries = inverse_rows(moment)
    result = jnp.zeros((SUB, LANES), jnp.float32)
    for j, entry in enumerate(entries):
        result = jnp.where(line == j, entry, result)
    mom_ref[...] = result
    for d in range(1, nc):
        mom_send(d).wait_send()
    for c in range(parts):
        for s in range(steps):
            half_send(c, s).wait_send()
    for t in range(tiles):
        block_keep(t).wait()
        for d in range(1, nb):
            block_send(t, d).wait()


def turn_kernel(inv_ref, in_ref, tay_ref, out_ref, comp_ref):
    many, outer = in_ref.shape[2], in_ref.shape[3]
    for k in range(many):
        out_ref[0, 0, pl.ds(k * outer, outer), :] = in_ref[0, :, k, :].T
    aa, ab, ac, bb, bc, cc = (inv_ref[j, 0] for j in range(6))
    for t, row in enumerate(((aa, ab, ac), (ab, bb, bc), (ac, bc, cc))):
        comp_ref[t] = row[0] * tay_ref[0] + row[1] * tay_ref[1] + row[2] * tay_ref[2]


def local(nc, nb, residual, weight_index, weight_table, gridded):
    count, row_count, columns = residual.shape
    _, groups, rows, length = gridded.shape
    outer = length // LANES
    tiles, parts = rows // SUB, row_count // SUB
    wide = columns // nc
    kept = LANES // nb
    steps = int(math.log2(nc))
    view = gridded.reshape(2, tiles, SUB, outer, LANES)
    view = jnp.transpose(view, (0, 1, 3, 2, 4)).reshape(2, tiles, outer * SUB, LANES)
    vmem = pl.BlockSpec(memory_space=pltpu.VMEM)
    smem = pl.BlockSpec(memory_space=pltpu.SMEM)
    hbm = pl.BlockSpec(memory_space=pl.ANY)
    dma = pltpu.SemaphoreType.DMA
    raw, taylor, moment = pl.pallas_call(
        functools.partial(exchange_kernel, nc, nb),
        out_shape=(
            jax.ShapeDtypeStruct((2, nb * rows, kept, outer), jnp.float32),
            jax.ShapeDtypeStruct((3, parts, SUB, wide), jnp.float32),
            jax.ShapeDtypeStruct((SUB, LANES), jnp.float32),
        ),
        in_specs=[smem, smem, vmem, vmem, vmem, vmem, hbm, hbm],
        out_specs=(hbm, vmem, vmem),
        scratch_shapes=[
            pltpu.VMEM((2, tiles, outer * SUB, LANES), jnp.float32),
            pltpu.VMEM((2, rows, LANES, outer), jnp.float32),
            pltpu.VMEM((parts, count, SUB, columns), jnp.float32),
            pltpu.VMEM((parts, nc, 3 * SUB, wide), jnp.float32),
            pltpu.VMEM((SUB, LANES), jnp.float32),
            pltpu.VMEM((nc - 1, SUB, LANES), jnp.float32),
            *[
                pltpu.VMEM((parts, nc >> (s + 1), 3 * SUB, wide), jnp.float32)
                for s in range(steps)
            ],
            dma((tiles,)),
            dma((parts,)),
            dma((tiles,)),
            dma((tiles, nb - 1)),
            dma((tiles, nb - 1)),
            dma((parts, steps)),
            dma((parts, steps)),
            dma((nc - 1,)),
            dma((nc - 1,)),
        ],
        compiler_params=pltpu.CompilerParams(
            collective_id=0, has_side_effects=True, vmem_limit_bytes=60 * 1024 * 1024
        ),
        name="exchange",
    )(weight_index, weight_table, *map(jnp.asarray, tables(length)), residual, view)
    many = min(SUB, kept)
    cuts = 2 * (kept // many)
    piece = pl.BlockSpec(
        (3, row_count, wide // cuts), lambda p, k: (0, 0, p * (kept // many) + k)
    )
    spectrum, components = pl.pallas_call(
        turn_kernel,
        grid=(2, kept // many),
        out_shape=(
            jax.ShapeDtypeStruct((2, 1, kept * outer, nb * rows), jnp.float32),
            jax.ShapeDtypeStruct((3, row_count, wide), jnp.float32),
        ),
        in_specs=[
            smem,
            pl.BlockSpec((1, nb * rows, many, outer), lambda p, k: (p, 0, k, 0)),
            piece,
        ],
        out_specs=(
            pl.BlockSpec((1, 1, many * outer, nb * rows), lambda p, k: (p, 0, k, 0)),
            piece,
        ),
        name="turn",
    )(moment, raw, taylor.reshape(3, row_count, wide))
    return (components, spectrum)


def solution(mesh):
    nc, nb = mesh.shape["chan"], mesh.shape["band"]
    in_specs = (P("chan", "band", None), P("chan"), P(), P(None, "chan", "band", None))
    out_specs = (P(None, "band", "chan"), P(None, "chan", "band", None))
    return jax.shard_map(
        functools.partial(local, nc, nb),
        mesh=mesh,
        in_specs=in_specs,
        out_specs=out_specs,
        check_vma=False,
    )
```

```python
import functools
import math

import jax
import jax.numpy as jnp
import numpy as np
from jax import lax
from jax.experimental import pallas as pl
from jax.experimental.pallas import tpu as pltpu
from jax.sharding import PartitionSpec as P

MESH = pl.DeviceIdType.MESH
LANES = 128
SUB = 8


def block_form(table):
    real = np.block([[table.real, -table.imag], [table.imag, table.real]]).astype(np.float32)
    high = real.astype(jnp.bfloat16)
    low = (real - high.astype(np.float32)).astype(jnp.bfloat16)
    return np.concatenate([high, low, high], axis=1)


def dft(size):
    grid = np.outer(np.arange(size), np.arange(size)) % size
    return np.exp(-2j * np.pi * grid / size)


def tables(length):
    outer = length // LANES
    turn = np.exp(-2j * np.pi * np.outer(np.arange(outer), np.arange(LANES)) / length)
    turn = turn / math.sqrt(length)
    return (
        block_form(dft(outer)),
        block_form(dft(LANES)),
        turn.real.astype(np.float32),
        turn.imag.astype(np.float32),
    )


def inverse_rows(moment):
    s0, s1, s2, s3, s4 = (moment[j : j + 1, :] for j in range(5))
    aa = s2 * s4 - s3 * s3
    ab = s2 * s3 - s1 * s4
    ac = s1 * s3 - s2 * s2
    bb = s0 * s4 - s2 * s2
    bc = s1 * s2 - s0 * s3
    cc = s0 * s2 - s1 * s1
    determ = s0 * aa + s1 * ab + s2 * ac
    return [entry / determ for entry in (aa, ab, ac, bb, bc, cc)]


def exchange_kernel(
    nc,
    nb,
    idx_ref,
    tab_ref,
    first_ref,
    second_ref,
    turn_re_ref,
    turn_im_ref,
    res_hbm,
    grid_hbm,
    spec_hbm,
    tay_ref,
    mom_ref,
    grid_v,
    out_v,
    res_v,
    part_v,
    mom_own,
    mom_all,
    *rest,
):
    steps = int(math.log2(nc))
    lands = rest[:steps]
    (grid_sem, res_sem, own_sem, fs_sem, fr_sem, rs_sem, rr_sem, ms_sem, mr_sem) = rest[steps:]
    chan = lax.axis_index("chan")
    band = lax.axis_index("band")
    tiles, outer8 = grid_v.shape[1], grid_v.shape[2]
    outer = outer8 // SUB
    rows = tiles * SUB
    kept = LANES // nb
    parts = res_v.shape[0]
    count = res_v.shape[1]
    wide = part_v.shape[3]
    chunks = part_v.shape[0]
    cuts = chunks // parts

    def grid_copy(t):
        return pltpu.make_async_copy(grid_hbm.at[:, t], grid_v.at[:, t], grid_sem.at[t])

    def res_copy(c):
        return pltpu.make_async_copy(
            res_hbm.at[:, pl.ds(c * SUB, SUB), :], res_v.at[c], res_sem.at[c]
        )

    order = max(tiles, parts)
    for i in range(order):
        if i < parts:
            res_copy(i).start()
        if i < tiles:
            grid_copy(i).start()

    barrier = pltpu.get_barrier_semaphore()
    for d in range(1, nc):
        peer = lax.rem(chan + d, nc)
        pl.semaphore_signal(barrier, inc=1, device_id=(peer, band), device_id_type=MESH)
    for d in range(1, nb):
        peer = lax.rem(band + d, nb)
        pl.semaphore_signal(barrier, inc=1, device_id=(chan, peer), device_id_type=MESH)

    total = count * nc
    coeffs = []
    moments = [jnp.float32(0.0)] * 5
    for c in range(count):
        weight = tab_ref[idx_ref[c]]
        position = (chan * count + c).astype(jnp.float32)
        offset = (2.0 * position + 1.0) * (1.0 / total) - 1.0
        power = weight
        trio = []
        for j in range(5):
            if j < 3:
                trio.append(power)
            moments[j] = moments[j] + power
            power = power * offset
        coeffs.append(trio)
    line = lax.broadcasted_iota(jnp.int32, (SUB, LANES), 0)
    tile = jnp.zeros((SUB, LANES), jnp.float32)
    for j in range(5):
        tile = jnp.where(line == j, moments[j], tile)
    mom_own[...] = tile

    def transform(t):
        def pair(i, carry):
            cols = []
            for k in range(2):
                r = i * 2 + k
                cols.append(
                    jnp.concatenate(
                        [grid_v[p, t, pl.ds(r, outer, stride=SUB), :] for p in range(2)], axis=0
                    )
                )
            x = jnp.concatenate(cols, axis=1)
            high = x.astype(jnp.bfloat16)
            low = (x - high.astype(jnp.float32)).astype(jnp.bfloat16)
            mid = jnp.dot(
                first_ref[...],
                jnp.concatenate([high, high, low], axis=0),
                preferred_element_type=jnp.float32,
            )
            turn_re, turn_im = turn_re_ref[...], turn_im_ref[...]
            turned = []
            for k in range(2):
                re = mid[:outer, k * LANES : (k + 1) * LANES]
                im = mid[outer:, k * LANES : (k + 1) * LANES]
                turned.append(
                    jnp.concatenate(
                        [re * turn_re - im * turn_im, re * turn_im + im * turn_re], axis=1
                    )
                )
            y = jnp.concatenate(turned, axis=0)
            high = y.astype(jnp.bfloat16)
            low = (y - high.astype(jnp.float32)).astype(jnp.bfloat16)
            out = lax.dot_general(
                second_ref[...],
                jnp.concatenate([high, high, low], axis=1),
                (((1,), (1,)), ((), ())),
                preferred_element_type=jnp.float32,
            )
            for k in range(2):
                for p in range(2):
                    out_v[p, t * SUB + i * 2 + k] = out[
                        p * LANES : (p + 1) * LANES, k * outer : (k + 1) * outer
                    ]
            return carry

        lax.fori_loop(0, SUB // 2, pair, 0)

    def block_send(t, d):
        peer = lax.rem(band + d, nb)
        return pltpu.make_async_remote_copy(
            src_ref=out_v.at[:, pl.ds(t * SUB, SUB), pl.ds(peer * kept, kept), :],
            dst_ref=spec_hbm.at[:, pl.ds(band * rows + t * SUB, SUB), :, :],
            send_sem=fs_sem.at[t, d - 1],
            recv_sem=fr_sem.at[t, d - 1],
            device_id=(chan, peer),
            device_id_type=MESH,
        )

    def block_keep(t):
        return pltpu.make_async_copy(
            out_v.at[:, pl.ds(t * SUB, SUB), pl.ds(band * kept, kept), :],
            spec_hbm.at[:, pl.ds(band * rows + t * SUB, SUB), :, :],
            own_sem.at[t],
        )

    def weigh(c):
        step = 512 if wide % 512 == 0 else LANES

        def one(j, carry):
            spot = 0
            for s in range(steps):
                spot = spot + ((j // (1 << s)) % 2) * (1 << (steps - 1 - s))
            for q in range(wide // step):
                col = pl.multiple_of((j * cuts + c % cuts) * wide + q * step, LANES)
                sums = [None] * 3
                for ch in range(count):
                    x = res_v[c // cuts, ch, :, pl.ds(col, step)]
                    for t in range(3):
                        term = coeffs[ch][t] * x
                        sums[t] = term if ch == 0 else sums[t] + term
                for t in range(3):
                    part_v[c, spot, pl.ds(t * SUB, SUB), pl.ds(q * step, step)] = sums[t]
            return carry

        lax.fori_loop(0, nc, one, 0)

    bits = [(chan // (1 << s)) % 2 for s in range(steps)]
    partners = [chan + (1 - 2 * bits[s]) * (1 << s) for s in range(steps)]
    starts = [0]
    for s in range(steps):
        starts.append(starts[s] + bits[s] * (nc >> (s + 1)))

    def half_send(c, s):
        size = nc >> (s + 1)
        begin = starts[s] + (1 - bits[s]) * size
        return pltpu.make_async_remote_copy(
            src_ref=part_v.at[c, pl.ds(begin, size)],
            dst_ref=lands[s].at[c],
            send_sem=rs_sem.at[c, s],
            recv_sem=rr_sem.at[c, s],
            device_id=(partners[s], band),
            device_id_type=MESH,
        )

    def half_add(c, s, send=True):
        half_send(c, s).wait_recv()
        size = nc >> (s + 1)
        if s == steps - 1:
            for t in range(3):
                span = pl.ds(t * SUB, SUB)
                tay_ref[t, c // cuts, :, pl.ds(c % cuts * wide, wide)] = part_v[c, starts[s + 1], span, :] + lands[s][c, 0, span, :]
            return
        half = size // 2
        for mine in (1 - bits[s + 1], bits[s + 1]):
            for q in range(half):
                at = mine * half + q
                part_v[c, starts[s + 1] + at] = part_v[c, starts[s + 1] + at] + lands[s][c, at]
            if send and mine is not bits[s + 1]:
                half_send(c, s + 1).start()

    def mom_send(d):
        peer = lax.rem(chan + d, nc)
        return pltpu.make_async_remote_copy(
            src_ref=mom_own,
            dst_ref=mom_all.at[d - 1],
            send_sem=ms_sem.at[d - 1],
            recv_sem=mr_sem.at[d - 1],
            device_id=(peer, band),
            device_id_type=MESH,
        )

    ahead = min(2, chunks)
    moved = 0

    def advance(limit):
        nonlocal moved
        while moved < limit:
            half_add(moved, 1)
            if moved + ahead < chunks:
                half_send(moved + ahead, 1).start()
            moved += 1

    for i in range(order):
        if i < parts:
            res_copy(i).wait()
            for c in range(i * cuts, (i + 1) * cuts):
                weigh(c)
                if c == 0:
                    pl.semaphore_wait(barrier, nc + nb - 2)
                half_send(c, 0).start()
        if i < tiles:
            grid_copy(i).wait()
            transform(i)
            for d in range(1, nb):
                block_send(i, d).start()
            block_keep(i).start()
        if i < parts:
            for c in range(i * cuts, (i + 1) * cuts):
                half_add(c, 0, send=c < ahead)
        if i >= 1:
            advance(min(i, (min(i + 1, parts)) * cuts - ahead))
    for d in range(1, nc):
        mom_send(d).start()
    advance(chunks)
    for s in range(2, steps):
        for c in range(chunks):
            half_add(c, s)
    moment = mom_own[...]
    for d in range(1, nc):
        mom_send(d).wait_recv()
        moment = moment + mom_all[d - 1]
    entries = inverse_rows(moment)
    result = jnp.zeros((SUB, LANES), jnp.float32)
    for j, entry in enumerate(entries):
        result = jnp.where(line == j, entry, result)
    mom_ref[...] = result
    for d in range(1, nc):
        mom_send(d).wait_send()
    for c in range(chunks):
        for s in range(steps):
            half_send(c, s).wait_send()
    for t in range(tiles):
        block_keep(t).wait()
        for d in range(1, nb):
            block_send(t, d).wait()


def turn_kernel(inv_ref, in_ref, tay_ref, out_ref, comp_ref):
    many, outer = in_ref.shape[2], in_ref.shape[3]
    for k in range(many):
        out_ref[0, 0, pl.ds(k * outer, outer), :] = in_ref[0, :, k, :].T
    aa, ab, ac, bb, bc, cc = (inv_ref[j, 0] for j in range(6))
    for t, row in enumerate(((aa, ab, ac), (ab, bb, bc), (ac, bc, cc))):
        comp_ref[t] = row[0] * tay_ref[0] + row[1] * tay_ref[1] + row[2] * tay_ref[2]


def local(nc, nb, residual, weight_index, weight_table, gridded):
    count, row_count, columns = residual.shape
    _, groups, rows, length = gridded.shape
    outer = length // LANES
    tiles, parts = rows // SUB, row_count // SUB
    wide = columns // nc
    halves = 2
    kept = LANES // nb
    steps = int(math.log2(nc))
    view = gridded.reshape(2, tiles, SUB, outer, LANES)
    view = jnp.transpose(view, (0, 1, 3, 2, 4)).reshape(2, tiles, outer * SUB, LANES)
    vmem = pl.BlockSpec(memory_space=pltpu.VMEM)
    smem = pl.BlockSpec(memory_space=pltpu.SMEM)
    hbm = pl.BlockSpec(memory_space=pl.ANY)
    dma = pltpu.SemaphoreType.DMA
    raw, taylor, moment = pl.pallas_call(
        functools.partial(exchange_kernel, nc, nb),
        out_shape=(
            jax.ShapeDtypeStruct((2, nb * rows, kept, outer), jnp.float32),
            jax.ShapeDtypeStruct((3, parts, SUB, wide), jnp.float32),
            jax.ShapeDtypeStruct((SUB, LANES), jnp.float32),
        ),
        in_specs=[smem, smem, vmem, vmem, vmem, vmem, hbm, hbm],
        out_specs=(hbm, vmem, vmem),
        scratch_shapes=[
            pltpu.VMEM((2, tiles, outer * SUB, LANES), jnp.float32),
            pltpu.VMEM((2, rows, LANES, outer), jnp.float32),
            pltpu.VMEM((parts, count, SUB, columns), jnp.float32),
            pltpu.VMEM((parts * halves, nc, 3 * SUB, wide // halves), jnp.float32),
            pltpu.VMEM((SUB, LANES), jnp.float32),
            pltpu.VMEM((nc - 1, SUB, LANES), jnp.float32),
            *[
                pltpu.VMEM((parts * halves, nc >> (s + 1), 3 * SUB, wide // halves), jnp.float32)
                for s in range(steps)
            ],
            dma((tiles,)),
            dma((parts,)),
            dma((tiles,)),
            dma((tiles, nb - 1)),
            dma((tiles, nb - 1)),
            dma((parts * halves, steps)),
            dma((parts * halves, steps)),
            dma((nc - 1,)),
            dma((nc - 1,)),
        ],
        compiler_params=pltpu.CompilerParams(
            collective_id=0, has_side_effects=True, vmem_limit_bytes=60 * 1024 * 1024
        ),
        name="exchange",
    )(weight_index, weight_table, *map(jnp.asarray, tables(length)), residual, view)
    many = min(2 * SUB, kept)
    cuts = 2 * (kept // many)
    piece = pl.BlockSpec(
        (3, row_count, wide // cuts), lambda p, k: (0, 0, p * (kept // many) + k)
    )
    spectrum, components = pl.pallas_call(
        turn_kernel,
        grid=(2, kept // many),
        out_shape=(
            jax.ShapeDtypeStruct((2, 1, kept * outer, nb * rows), jnp.float32),
            jax.ShapeDtypeStruct((3, row_count, wide), jnp.float32),
        ),
        in_specs=[
            smem,
            pl.BlockSpec((1, nb * rows, many, outer), lambda p, k: (p, 0, k, 0)),
            piece,
        ],
        out_specs=(
            pl.BlockSpec((1, 1, many * outer, nb * rows), lambda p, k: (p, 0, k, 0)),
            piece,
        ),
        name="turn",
    )(moment, raw, taylor.reshape(3, row_count, wide))
    return (components, spectrum)


def solution(mesh):
    nc, nb = mesh.shape["chan"], mesh.shape["band"]
    in_specs = (P("chan", "band", None), P("chan"), P(), P(None, "chan", "band", None))
    out_specs = (P(None, "band", "chan"), P(None, "chan", "band", None))
    return jax.shard_map(
        functools.partial(local, nc, nb),
        mesh=mesh,
        in_specs=in_specs,
        out_specs=out_specs,
        check_vma=False,
    )
```
